32 devices in a mesh: tm: 2 (over y), lat: 4 (over x, core), lon: 4 (over z).
Axes of the slice: x: 2, y: 2, z: 4, core: 2. Of those that a mesh axis runs over, the one named last changes fastest.
Arguments:
- increments: float32 [2, 16, 32, 1536], P('tm', None, 'lat', 'lon'), may hold values from -6 to 6
- advection: float32 [16, 32, 1536], P(None, 'lat', 'lon'), may hold values from 0.2 to 0.4
- diffusion: float32 [16, 32, 1536], P(None, 'lat', 'lon'), may hold values from 0.25 to 0.3
- departures: float32 [2, 6, 16, 32, 1536], P('tm', None, None, 'lat', 'lon'), may hold values from -6 to 6
- obs_weight: float32 [16], replicated, may hold values from 0.5 to 2
- error_weight: float32 [16], replicated, may hold values from 0.5 to 2
- penalty_weight: float32 [16], replicated, may hold values from 0.5 to 2
- filter_steps: int32 [6], replicated, may hold values from 0 to 11, as said below
- filter_weights: float32 [6], replicated, may hold values from 0.05 to 0.3
Outputs:
- gradient: float32 [2, 16, 32, 1536], P('tm', None, 'lat', 'lon')
The draws below stay inside these ranges and needn't reach their ends.
Inputs may be any that keep to these rules, and one draw needn't show every extreme that they name: filter_steps lists, for k = 0 .. 1 in turn, 3 different steps of subwindow k, each in k * 6 to k * 6 + 5.
All inputs are finite; a program needn't handle non-finite values.
Results may differ from the reference program's by a relative error of at most 0.00002.
Values sent between devices are 32-bit elements; how exact they have to be, the bound alone decides.
No kernel may reach another device: no remote copies, remote signals or barrier semaphores. Data moves between devices by JAX's collectives and lax.ppermute only.
A program may use at most 64 MiB of HBM per device.

```python
import math
import jax
import jax.numpy as jnp

LEV = 16
STEPS = 6
TAPS_SUB = 3
SUBS = 2
TAPS = 6
NLAT = 32
NLON = 1536


def draw_filter_steps(key, part):
    subkeys = jax.random.split(jax.random.fold_in(key, 7), SUBS)

    def choose(subkey):
        return jax.random.permutation(subkey, STEPS)[:TAPS_SUB]
    chosen = jax.vmap(choose)(subkeys)
    offsets = STEPS * jnp.arange(SUBS, dtype=jnp.int32)
    return (chosen.astype(jnp.int32) + offsets[:, None]).reshape(-1).astype(jnp.int32)


def steps_of(key, shape, cuts, smallest, high):
    def one(dim, blocks):
        draws = jax.random.uniform(jax.random.fold_in(jax.random.fold_in(key, 6), dim), (blocks,), jnp.float32, smallest / len(cuts), high / len(cuts))
        return jnp.repeat(jnp.exp(draws), shape[dim] // blocks).reshape((-1,) + (1,) * (len(shape) - dim - 1))

    factor_of = one(*cuts[0])
    for cut in cuts[1:]:
        factor_of = factor_of * one(*cut)
    return factor_of


def scatter_about(rng, dims, width, limit, shards=(), kind=jnp.bfloat16):
    drawn = jax.random.normal(rng, dims, jnp.float32) * width
    if len(shards) > 0:
        drawn = steps_of(rng, dims, shards, -0.22, 0.18) * drawn
    return jnp.clip(drawn, min=-limit, max=limit).astype(kind)


def setup_inputs(seed: int = 0) -> dict:
    streams_of = jax.random.split(jax.random.key(seed), 10)
    return {
        "increments": scatter_about(streams_of[0], (SUBS, LEV, NLAT, NLON), 1.0, 6.0, ((0, 2), (2, 4), (3, 4)), jnp.float32),
        "advection": jnp.clip(0.2 + 0.2 * jax.random.uniform(streams_of[1], (LEV, NLAT, NLON), jnp.float32) ** steps_of(streams_of[1], (LEV, NLAT, NLON), ((1, 4), (2, 4)), -0.2, 0.2), 0.2, 0.4),
        "diffusion": jnp.clip(0.25 + 0.050000012 * jax.random.uniform(streams_of[2], (LEV, NLAT, NLON), jnp.float32) ** steps_of(streams_of[2], (LEV, NLAT, NLON), ((1, 4), (2, 4)), -0.2, 0.2), 0.25, 0.3),
        "departures": scatter_about(streams_of[3], (SUBS, STEPS, LEV, NLAT, NLON), 1.0, 6.0, ((0, 2), (3, 4), (4, 4)), jnp.float32),
        "obs_weight": jnp.clip(jnp.exp(jax.random.uniform(streams_of[4], (LEV,), jnp.float32, math.log(0.5), math.log(2.0))), 0.5, 2.0),
        "error_weight": jnp.clip(jnp.exp(jax.random.uniform(streams_of[5], (LEV,), jnp.float32, math.log(0.5), math.log(2.0))), 0.5, 2.0),
        "penalty_weight": jnp.clip(jnp.exp(jax.random.uniform(streams_of[6], (LEV,), jnp.float32, math.log(0.5), math.log(2.0))), 0.5, 2.0),
        "filter_steps": draw_filter_steps(jax.random.fold_in(streams_of[9], 71), 0),
        "filter_weights": jnp.clip(jnp.exp(jax.random.uniform(streams_of[8], (TAPS,), jnp.float32, math.log(0.05), math.log(0.3))), 0.05, 0.3),
    }


def model_step(field, advection, diffusion):
    western = jnp.roll(field, 1, axis=2)
    padded = jnp.pad(field, ((0, 0), (1, 1), (0, 0)))
    meridian = padded[:, 2:, :] + padded[:, :-2, :]
    return (1.0 - advection - 2.0 * diffusion) * field + advection * western + diffusion * meridian


def adjoint_step(field, advection, diffusion):
    carried = advection * field
    spread = diffusion * field
    eastern = jnp.roll(carried, -1, axis=2)
    padded = jnp.pad(spread, ((0, 0), (1, 1), (0, 0)))
    meridian = padded[:, 2:, :] + padded[:, :-2, :]
    return (1.0 - advection - 2.0 * diffusion) * field + eastern + meridian


def reference(increments, advection, diffusion, departures, obs_weight, error_weight, penalty_weight, filter_steps, filter_weights):
    window = SUBS * STEPS
    middle = window // 2
    times = jnp.arange(window, dtype=jnp.int32)
    tap = jnp.sum(filter_weights[:, None] * (filter_steps[:, None] == times[None, :]).astype(jnp.float32), axis=0)
    coef = tap - (times == middle).astype(jnp.float32)
    obs_level = obs_weight[:, None, None]
    err_level = error_weight[:, None, None]
    filtered = jnp.zeros(increments.shape[1:], jnp.float32)
    finals = []
    for sub in range(SUBS):
        field = increments[sub]
        for step in range(STEPS):
            filtered = filtered + coef[sub * STEPS + step] * field
            field = model_step(field, advection, diffusion)
        finals.append(field)
    force = penalty_weight[:, None, None] * filtered
    mismatch = [increments[0]] + [increments[sub] - finals[sub - 1] for sub in range(1, SUBS)]
    outputs = []
    for sub in range(SUBS):
        states = []
        field = increments[sub]
        for step in range(STEPS):
            states.append(field)
            field = model_step(field, advection, diffusion)
        if sub + 1 < SUBS:
            adjoint = -err_level * mismatch[sub + 1]
        else:
            adjoint = jnp.zeros_like(field)
        for step in range(STEPS - 1, -1, -1):
            forcing = obs_level * (states[step] - departures[sub, step]) + coef[sub * STEPS + step] * force
            adjoint = forcing + adjoint_step(adjoint, advection, diffusion)
        scale = jnp.ones_like(err_level) if sub == 0 else err_level
        outputs.append(adjoint + scale * mismatch[sub])
    return jnp.stack(outputs)
```

```python
import functools
import jax
import jax.numpy as jnp
from jax import lax
from jax.experimental import pallas as pl
from jax.experimental.pallas import tpu as pltpu
from jax.sharding import PartitionSpec as P

LANES = 128
F32 = jnp.float32
VM = pl.BlockSpec(memory_space=pltpu.VMEM)
SM = pl.BlockSpec(memory_space=pltpu.SMEM)


def call(kernel, operands, specs, shapes, scratch=(), name=None):
    return pl.pallas_call(
        kernel,
        out_shape=[jax.ShapeDtypeStruct(s, F32) for s in shapes],
        in_specs=specs,
        out_specs=[VM] * len(shapes),
        scratch_shapes=list(scratch),
        name=name,
    )(*operands)


def slot_width(steps):
    width = 8
    while width < steps:
        width *= 2
    return width


def lane_slots(count, steps):
    per_tile = LANES // slot_width(steps)
    return -(-count // per_tile)


def pack_slots(tiles, levels, steps, first_lane):
    width = slot_width(steps)
    per_tile = LANES // width
    lane = lax.broadcasted_iota(jnp.int32, (levels, LANES), 1)
    packed = []
    for base in range(0, len(tiles), per_tile):
        acc = jnp.zeros((levels, LANES), F32)
        for slot, tile in enumerate(tiles[base : base + per_tile]):
            moved = pltpu.roll(tile(), (slot * width - first_lane) % LANES, 1)
            acc = jnp.where((lane >= slot * width) & (lane < slot * width + steps), moved, acc)
        packed.append(acc)
    return packed


def unpack_slot(packed_ref, index, levels, steps, first_lane):
    width = slot_width(steps)
    per_tile = LANES // width
    base, slot = divmod(index, per_tile)
    lane = lax.broadcasted_iota(jnp.int32, (levels, LANES), 1)
    tile = packed_ref[:, base * LANES : (base + 1) * LANES]
    moved = pltpu.roll(tile, (first_lane - slot * width) % LANES, 1)
    return jnp.where((lane >= first_lane) & (lane < first_lane + steps), moved, 0.0)


def read_row(ref, levels, rows, r, base=0):
    tiles = ref.shape[0] // (levels * rows) if not base else base[1]
    start = base[0] * levels * rows * tiles if base else 0
    return jnp.concatenate(
        [ref[pl.ds(start + c * rows + r, levels, stride=rows * tiles), :] for c in range(tiles)], axis=1
    )


def tiled(block):
    *lead, rows, cols = block.shape
    split = block.reshape((*lead, rows, cols // LANES, LANES))
    return jnp.swapaxes(split, -3, -2).reshape((-1, LANES))


def untiled(flat, levels, rows, cols):
    split = flat.reshape((levels, cols // LANES, rows, LANES))
    return jnp.swapaxes(split, 1, 2).reshape((levels, rows, cols))


def pack_kernel(steps, rows, levels, x_ref, adv_ref, dif_ref, own_ref, up_ref, down_ref):
    halos = (steps, steps - 1, steps - 1)
    base = 0
    for field, ref in enumerate((x_ref, adv_ref, dif_ref)):
        halo = halos[field]
        for r in range(rows):
            value = read_row(ref, levels, rows, r)
            own_ref[field, r] = value
            if r < halo:
                down_ref[base + r] = value
            if r >= rows - halo:
                up_ref[base + r - (rows - halo)] = value
        base += halo


def row_source(steps, rows, field, row, own_ref, before_ref, after_ref):
    halo = (steps, steps - 1, steps - 1)[field]
    base = (0, steps, 2 * steps - 1)[field]
    if row < 0:
        return before_ref, (base + row + halo,)
    if row >= rows:
        return after_ref, (base + row - rows,)
    return own_ref, (field, row)


def wide_rows(steps, rows):
    listed = [(0, r) for r in range(-steps, rows + steps)]
    for field in (1, 2):
        listed += [(field, r) for r in range(-(steps - 1), rows + steps - 1)]
    return listed


def strip_kernel(steps, rows, levels, own_ref, before_ref, after_ref, out_ref):
    def tile(field, row):
        ref, index = row_source(steps, rows, field, row, own_ref, before_ref, after_ref)
        return lambda: ref[index + (slice(None), slice(-LANES, None))]

    packed = pack_slots(
        [tile(f, r) for f, r in wide_rows(steps, rows)], levels, steps, LANES - steps
    )
    for i, value in enumerate(packed):
        out_ref[:, i * LANES : (i + 1) * LANES] = value


def coefficients(position, middle, steps, taps_ref, weights_ref):
    found = []
    for s in range(steps):
        step = position * steps + s
        total = jnp.where(step == middle, -1.0, 0.0).astype(F32)
        for j in range(taps_ref.shape[0]):
            total = total + jnp.where(taps_ref[j] == step, weights_ref[j], 0.0)
        found.append(total)
    return found


def forward_kernel(
    steps, rows, levels, middle,
    position_ref, taps_ref, weights_ref, obs_ref, own_ref, before_ref, after_ref, strip_ref, dep_ref,
    adv_ref, dif_ref, keep_ref, forcing_ref, filt_ref, final_ref,
    a_ref, b_ref,
):
    cols = own_ref.shape[-1]
    wide = cols + LANES
    coef = coefficients(position_ref[0], middle, steps, taps_ref, weights_ref)
    obs = jnp.broadcast_to(obs_ref[...], (levels, cols))
    targets = (a_ref, adv_ref, dif_ref)
    for index, (field, row) in enumerate(wide_rows(steps, rows)):
        ref, where = row_source(steps, rows, field, row, own_ref, before_ref, after_ref)
        target = targets[field]
        target[row + steps, :, :LANES] = unpack_slot(strip_ref, index, levels, steps, LANES - steps)
        target[row + steps, :, LANES:] = ref[where]
    for ref in (adv_ref, dif_ref):
        for row in (0, rows + 2 * steps - 1):
            ref[row] = jnp.zeros((levels, wide), F32)
    for row in range(rows + 2 * steps):
        keep_ref[row] = 1.0 - adv_ref[row] - 2.0 * dif_ref[row]
    current, fresh = a_ref, b_ref
    for s in range(steps):
        for r in range(rows):
            state = current[r + steps, :, LANES:]
            departure = read_row(dep_ref, levels, rows, r, (s, cols // LANES))
            forcing_ref[s, r] = obs * (state - departure)
            if s == 0:
                filt_ref[r] = coef[s] * state
            else:
                filt_ref[r] = filt_ref[r] + coef[s] * state
        for row in range(s + 1, rows + 2 * steps - s - 1):
            here = current[row]
            western = pltpu.roll(here, 1, 1)
            meridian = current[row + 1] + current[row - 1]
            fresh[row] = keep_ref[row] * here + adv_ref[row] * western + dif_ref[row] * meridian
        current, fresh = fresh, current
    for r in range(rows):
        final_ref[r] = current[r + steps, :, LANES:]


def adjoint_kernel(
    steps, rows, levels, middle, members,
    position_ref, taps_ref, weights_ref, err_ref, pen_ref,
    adv_ref, dif_ref, keep_ref, forcing_ref, filt_ref, other_ref, final_ref, next_ref,
    main_ref, strip_ref,
    a_ref, b_ref, force_ref,
):
    cols = forcing_ref.shape[-1]
    wide = cols + LANES
    total_rows = rows + 2 * steps
    position = position_ref[0]
    coef = coefficients(position, middle, steps, taps_ref, weights_ref)
    linked = jnp.where(position == members - 1, 0.0, 1.0).astype(F32)
    err = jnp.broadcast_to(err_ref[...], (levels, cols)) * linked
    pen = jnp.broadcast_to(pen_ref[...], (levels, cols))
    zero = jnp.zeros((levels, wide), F32)
    for row in range(total_rows):
        if row < steps or row >= rows + steps:
            a_ref[row] = zero
            b_ref[row] = zero
    for r in range(rows):
        following = read_row(next_ref, levels, rows, r)
        a_ref[r + steps, :, :LANES] = zero[:, :LANES]
        a_ref[r + steps, :, LANES:] = err * (final_ref[r] - following)
        force_ref[r] = pen * (filt_ref[r] + other_ref[r])
    current, fresh = a_ref, b_ref
    for j in range(steps):
        s = steps - 1 - j
        for row in range(steps - j - 1, rows + steps + j + 1):
            here = current[row]
            value = keep_ref[row] * here + pltpu.roll(adv_ref[row] * here, wide - 1, 1)
            if row + 1 < total_rows:
                value = value + dif_ref[row + 1] * current[row + 1]
            if row >= 1:
                value = value + dif_ref[row - 1] * current[row - 1]
            r = row - steps
            if 0 <= r < rows:
                fresh[row, :, :LANES] = value[:, :LANES]
                fresh[row, :, LANES:] = value[:, LANES:] + (forcing_ref[s, r] + coef[s] * force_ref[r])
            else:
                fresh[row] = value
        current, fresh = fresh, current
    for row in range(total_rows):
        main_ref[row] = current[row, :, LANES:]
    packed = pack_slots(
        [functools.partial(lambda q: current[q, :, :LANES], row) for row in range(total_rows)],
        levels, steps, LANES - steps,
    )
    for i, value in enumerate(packed):
        strip_ref[:, i * LANES : (i + 1) * LANES] = value


def spill_kernel(steps, rows, levels, main_ref, strip_ref, up_ref, down_ref):
    for i in range(steps):
        for ref, row in ((down_ref, i), (up_ref, rows + steps + i)):
            ref[i, :, :-LANES] = main_ref[row, :, :-LANES]
            ref[i, :, -LANES:] = main_ref[row, :, -LANES:] + unpack_slot(
                strip_ref, row, levels, steps, LANES - steps
            )


def final_kernel(
    steps, rows, levels,
    position_ref, err_ref, main_ref, strip_ref, before_ref, after_ref, x_ref, previous_ref, out_ref,
):
    cols = main_ref.shape[-1]
    err = jnp.broadcast_to(err_ref[...], (levels, cols))
    scale = jnp.where(position_ref[0] == 0, jnp.ones_like(err), err)
    for r in range(rows):
        row = r + steps
        spilled = unpack_slot(strip_ref, row, levels, steps, LANES - steps)
        value = jnp.concatenate(
            [main_ref[row, :, :-LANES], main_ref[row, :, -LANES:] + spilled], axis=1
        )
        if r < steps:
            value = value + before_ref[r]
        if r >= rows - steps:
            value = value + after_ref[r - (rows - steps)]
        value = value + scale * (x_ref[r] - previous_ref[r])
        tiles = cols // LANES
        for c in range(tiles):
            out_ref[pl.ds(c * rows + r, levels, stride=rows * tiles), :] = value[:, c * LANES : (c + 1) * LANES]


def along(value, axis, by, ring=False):
    count = lax.axis_size(axis)
    if ring:
        return lax.ppermute(value, axis, [(i, (i + by) % count) for i in range(count)])
    return lax.ppermute(value, axis, [(i, i + by) for i in range(count) if 0 <= i + by < count])


def halves(value, axis):
    count = lax.axis_size(axis)
    if count & (count - 1):
        return lax.psum(value, axis), jnp.zeros_like(value)
    distance = 1
    other = jnp.zeros_like(value)
    while distance < count:
        if distance > 1:
            value = value + other
        other = lax.ppermute(value, axis, [(i, i ^ distance) for i in range(count)])
        distance *= 2
    return value, other


def body(
    increments, advection, diffusion, departures,
    obs_weight, error_weight, penalty_weight, filter_steps, filter_weights,
):
    members = lax.axis_size("tm")
    _, steps, levels, rows, cols = departures.shape
    middle = members * steps // 2
    position = lax.axis_index("tm").astype(jnp.int32)[None]
    obs, err, pen = (w[:, None] for w in (obs_weight, error_weight, penalty_weight))
    x, adv, dif, dep = (tiled(v) for v in (increments, advection, diffusion, departures))
    bind = functools.partial
    total_rows = rows + 2 * steps
    wide = cols + LANES
    halo_rows = 3 * steps - 2
    row_set = (levels, cols)

    own, up, down = call(
        bind(pack_kernel, steps, rows, levels), (x, adv, dif), [VM] * 3,
        [(3, rows) + row_set, (halo_rows,) + row_set, (halo_rows,) + row_set], name="pack",
    )
    before = along(up, "lat", 1)
    after = along(down, "lat", -1)
    following = along(x, "tm", -1)

    strip_shape = (levels, LANES * lane_slots(len(wide_rows(steps, rows)), steps))
    (strip,) = call(
        bind(strip_kernel, steps, rows, levels), (own, before, after), [VM] * 3, [strip_shape], name="strip",
    )
    strip = along(strip, "lon", 1, ring=True)

    wide_shape = (total_rows, levels, wide)
    adv_w, dif_w, keep_w, forcing, filt, final = call(
        bind(forward_kernel, steps, rows, levels, middle),
        (position, filter_steps, filter_weights, obs, own, before, after, strip, dep),
        [SM] * 3 + [VM] * 6,
        [wide_shape] * 3 + [(steps, rows) + row_set, (rows,) + row_set, (rows,) + row_set],
        [pltpu.VMEM(wide_shape, F32)] * 2, name="forward",
    )
    filt, other = halves(filt, "tm")
    previous = along(final, "tm", 1)

    main, spill = call(
        bind(adjoint_kernel, steps, rows, levels, middle, members),
        (position, filter_steps, filter_weights, err, pen, adv_w, dif_w, keep_w, forcing, filt, other, final, following),
        [SM] * 3 + [VM] * 10,
        [(total_rows,) + row_set, (levels, LANES * lane_slots(total_rows, steps))],
        [pltpu.VMEM(wide_shape, F32)] * 2 + [pltpu.VMEM((rows,) + row_set, F32)], name="adjoint",
    )
    spill = along(spill, "lon", -1, ring=True)
    up, down = call(
        bind(spill_kernel, steps, rows, levels), (main, spill), [VM] * 2, [(steps,) + row_set] * 2, name="spill",
    )
    before = along(up, "lat", 1)
    after = along(down, "lat", -1)
    (out,) = call(
        bind(final_kernel, steps, rows, levels),
        (position, err, main, spill, before, after, own[0], previous), [SM] + [VM] * 7, [x.shape], name="final",
    )
    return untiled(out, levels, rows, cols)[None]


def solution(mesh):
    return jax.shard_map(
        body,
        mesh=mesh,
        in_specs=(
            P("tm", None, "lat", "lon"),
            P(None, "lat", "lon"),
            P(None, "lat", "lon"),
            P("tm", None, None, "lat", "lon"),
            P(),
            P(),
            P(),
            P(),
            P(),
        ),
        out_specs=P("tm", None, "lat", "lon"),
        check_vma=False,
    )
```

```python
import functools
import jax
import jax.numpy as jnp
from jax import lax
from jax.experimental import pallas as pl
from jax.experimental.pallas import tpu as pltpu
from jax.sharding import PartitionSpec as P

LANES = 128
F32 = jnp.float32
SCOPED = 16 * 2**20
VM = pl.BlockSpec(memory_space=pltpu.VMEM)
SM = pl.BlockSpec(memory_space=pltpu.SMEM)
HB = pl.BlockSpec(memory_space=pltpu.HBM)


def call(kernel, operands, specs, shapes, scratch=(), name=None, kept=True):
    operands = [
        pltpu.with_memory_space_constraint(o, pltpu.VMEM if spec is VM else pltpu.HBM) if spec is not SM else o
        for o, spec in zip(operands, specs, strict=True)
    ]
    return pl.pallas_call(
        kernel,
        out_shape=[pltpu.VMEM(s, F32) if kept else jax.ShapeDtypeStruct(s, F32) for s in shapes],
        in_specs=specs,
        out_specs=[VM] * len(shapes),
        scratch_shapes=list(scratch),
        compiler_params=pltpu.CompilerParams(vmem_limit_bytes=SCOPED),
        name=name,
    )(*operands)


def slot_width(steps):
    width = 8
    while width < steps:
        width *= 2
    return width


def lane_slots(count, steps):
    per_tile = LANES // slot_width(steps)
    return -(-count // per_tile)


def pack_slots(tiles, levels, steps, first_lane):
    width = slot_width(steps)
    per_tile = LANES // width
    lane = lax.broadcasted_iota(jnp.int32, (levels, LANES), 1)
    packed = []
    for base in range(0, len(tiles), per_tile):
        acc = jnp.zeros((levels, LANES), F32)
        for slot, tile in enumerate(tiles[base : base + per_tile]):
            moved = pltpu.roll(tile(), (slot * width - first_lane) % LANES, 1)
            acc = jnp.where((lane >= slot * width) & (lane < slot * width + steps), moved, acc)
        packed.append(acc)
    return packed


def unpack_slot(packed_ref, index, levels, steps, first_lane):
    width = slot_width(steps)
    per_tile = LANES // width
    base, slot = divmod(index, per_tile)
    lane = lax.broadcasted_iota(jnp.int32, (levels, LANES), 1)
    tile = packed_ref[:, base * LANES : (base + 1) * LANES]
    moved = pltpu.roll(tile, (first_lane - slot * width) % LANES, 1)
    return jnp.where((lane >= first_lane) & (lane < first_lane + steps), moved, 0.0)


def read_row(ref, levels, rows, r, base=0):
    tiles = ref.shape[0] // (levels * rows) if not base else base[1]
    start = base[0] * levels * rows * tiles if base else 0
    return jnp.concatenate(
        [ref[pl.ds(start + c * rows + r, levels, stride=rows * tiles), :] for c in range(tiles)], axis=1
    )


def tiled(block):
    *lead, rows, cols = block.shape
    split = block.reshape((*lead, rows, cols // LANES, LANES))
    return jnp.swapaxes(split, -3, -2).reshape((-1, LANES))


def untiled(flat, levels, rows, cols):
    split = flat.reshape((levels, cols // LANES, rows, LANES))
    return jnp.swapaxes(split, 1, 2).reshape((levels, rows, cols))


def pack_kernel(
    steps, rows, levels,
    odd_ref, x_ref, adv_ref, dif_ref, own_ref, far_ref, near_ref, landing_ref, arrived,
):
    odd = jnp.full((levels, own_ref.shape[-1]), odd_ref[0]) == 1
    halos = (steps, steps - 1, steps - 1)
    base = 0
    copies = [
        pltpu.make_async_copy(ref, landing_ref.at[field], arrived.at[field])
        for field, ref in enumerate((x_ref, adv_ref, dif_ref))
    ]
    for copy in copies:
        copy.start()
    for field, copy in enumerate(copies):
        copy.wait()
        ref = landing_ref.at[field]
        halo = halos[field]
        values = [read_row(ref, levels, rows, r) for r in range(rows)]
        for r in range(rows):
            own_ref[field, r] = values[r]
        for q in range(halo):
            down, up = values[q], values[rows - halo + q]
            far_ref[base + q] = jnp.where(odd, up, down)
            near_ref[base + q] = jnp.where(odd, down, up)
        base += halo


def row_source(steps, rows, field, row, odd, own_ref, far_ref, near_ref):
    halo = (steps, steps - 1, steps - 1)[field]
    base = (0, steps, 2 * steps - 1)[field]
    if row < 0:
        q = base + row + halo
        return lambda cols: jnp.where(odd, near_ref[q, :, cols], far_ref[q, :, cols])
    if row >= rows:
        q = base + row - rows
        return lambda cols: jnp.where(odd, far_ref[q, :, cols], near_ref[q, :, cols])
    return lambda cols: own_ref[field, row, :, cols]


def wide_rows(steps, rows):
    listed = [(0, r) for r in range(-steps, rows + steps)]
    for field in (1, 2):
        listed += [(field, r) for r in range(-(steps - 1), rows + steps - 1)]
    return listed


def strip_kernel(steps, rows, levels, odd_ref, own_ref, far_ref, near_ref, out_ref):
    odd = jnp.full((levels, LANES), odd_ref[0]) == 1

    def tile(field, row):
        read = row_source(steps, rows, field, row, odd, own_ref, far_ref, near_ref)
        return lambda: read(slice(-LANES, None))

    packed = pack_slots(
        [tile(f, r) for f, r in wide_rows(steps, rows)], levels, steps, LANES - steps
    )
    for i, value in enumerate(packed):
        out_ref[:, i * LANES : (i + 1) * LANES] = value


def per_level(ref, levels, cols):
    level = lax.broadcasted_iota(jnp.int32, (levels, cols), 0)
    value = jnp.zeros((levels, cols), F32)
    for i in range(levels):
        value = jnp.where(level == i, ref[i], value)
    return value


def coefficients(position, middle, steps, taps_ref, weights_ref):
    found = []
    for s in range(steps):
        step = position * steps + s
        total = jnp.where(step == middle, -1.0, 0.0).astype(F32)
        for j in range(taps_ref.shape[0]):
            total = total + jnp.where(taps_ref[j] == step, weights_ref[j], 0.0)
        found.append(total)
    return found


def forward_kernel(
    steps, rows, levels, middle,
    position_ref, odd_ref, taps_ref, weights_ref, obs_ref, own_ref, far_ref, near_ref, strip_ref, dep_ref,
    adv_ref, dif_ref, keep_ref, forcing_ref, filt_ref, final_ref,
    a_ref, b_ref,
):
    cols = own_ref.shape[-1]
    wide = cols + LANES
    coef = coefficients(position_ref[0], middle, steps, taps_ref, weights_ref)
    obs = per_level(obs_ref, levels, cols)
    odd = jnp.full((levels, cols), odd_ref[0]) == 1
    targets = (a_ref, adv_ref, dif_ref)
    for index, (field, row) in enumerate(wide_rows(steps, rows)):
        read = row_source(steps, rows, field, row, odd, own_ref, far_ref, near_ref)
        target = targets[field]
        target[row + steps, :, :LANES] = unpack_slot(strip_ref, index, levels, steps, LANES - steps)
        target[row + steps, :, LANES:] = read(slice(None))
    for ref in (adv_ref, dif_ref):
        for row in (0, rows + 2 * steps - 1):
            ref[row] = jnp.zeros((levels, wide), F32)
    for row in range(rows + 2 * steps):
        keep_ref[row] = 1.0 - adv_ref[row] - 2.0 * dif_ref[row]
    current, fresh = a_ref, b_ref
    for s in range(steps):
        for r in range(rows):
            state = current[r + steps, :, LANES:]
            departure = read_row(dep_ref, levels, rows, r, (s, cols // LANES))
            forcing_ref[s, r] = obs * (state - departure)
            if s == 0:
                filt_ref[r] = coef[s] * state
            else:
                filt_ref[r] = filt_ref[r] + coef[s] * state
        for row in range(s + 1, rows + 2 * steps - s - 1):
            here = current[row]
            western = pltpu.roll(here, 1, 1)
            meridian = current[row + 1] + current[row - 1]
            fresh[row] = keep_ref[row] * here + adv_ref[row] * western + dif_ref[row] * meridian
        current, fresh = fresh, current
    for r in range(rows):
        final_ref[r] = current[r + steps, :, LANES:]


def adjoint_kernel(
    steps, rows, levels, middle, members,
    position_ref, taps_ref, weights_ref, err_ref, pen_ref,
    adv_ref, dif_ref, keep_ref, forcing_ref, filt_ref, other_ref, final_ref, next_ref,
    main_ref, strip_ref,
    a_ref, b_ref, force_ref,
):
    cols = forcing_ref.shape[-1]
    wide = cols + LANES
    total_rows = rows + 2 * steps
    position = position_ref[0]
    coef = coefficients(position, middle, steps, taps_ref, weights_ref)
    linked = jnp.where(position == members - 1, 0.0, 1.0).astype(F32)
    err = per_level(err_ref, levels, cols) * linked
    pen = per_level(pen_ref, levels, cols)
    zero = jnp.zeros((levels, wide), F32)
    for row in range(total_rows):
        if row < steps or row >= rows + steps:
            a_ref[row] = zero
            b_ref[row] = zero
    for r in range(rows):
        following = read_row(next_ref, levels, rows, r)
        a_ref[r + steps, :, :LANES] = zero[:, :LANES]
        a_ref[r + steps, :, LANES:] = err * (final_ref[r] - following)
        force_ref[r] = pen * (filt_ref[r] + other_ref[r])
    current, fresh = a_ref, b_ref
    for j in range(steps):
        s = steps - 1 - j
        for row in range(steps - j - 1, rows + steps + j + 1):
            here = current[row]
            value = keep_ref[row] * here + pltpu.roll(adv_ref[row] * here, wide - 1, 1)
            if row + 1 < total_rows:
                value = value + dif_ref[row + 1] * current[row + 1]
            if row >= 1:
                value = value + dif_ref[row - 1] * current[row - 1]
            r = row - steps
            if 0 <= r < rows:
                fresh[row, :, :LANES] = value[:, :LANES]
                fresh[row, :, LANES:] = value[:, LANES:] + (forcing_ref[s, r] + coef[s] * force_ref[r])
            else:
                fresh[row] = value
        current, fresh = fresh, current
    for row in range(total_rows):
        main_ref[row] = current[row, :, LANES:]
    packed = pack_slots(
        [functools.partial(lambda q: current[q, :, :LANES], row) for row in range(total_rows)],
        levels, steps, LANES - steps,
    )
    for i, value in enumerate(packed):
        strip_ref[:, i * LANES : (i + 1) * LANES] = value


def spill_kernel(steps, rows, levels, odd_ref, main_ref, strip_ref, far_ref, near_ref):
    odd = jnp.full((levels, main_ref.shape[-1]), odd_ref[0]) == 1

    def full(row):
        spilled = unpack_slot(strip_ref, row, levels, steps, LANES - steps)
        return jnp.concatenate(
            [main_ref[row, :, :-LANES], main_ref[row, :, -LANES:] + spilled], axis=1
        )

    for q in range(steps):
        down, up = full(q), full(rows + steps + q)
        far_ref[q] = jnp.where(odd, up, down)
        near_ref[q] = jnp.where(odd, down, up)


def final_kernel(
    steps, rows, levels,
    position_ref, odd_ref, err_ref, main_ref, strip_ref, far_ref, near_ref, own_ref, previous_ref, out_ref,
):
    cols = main_ref.shape[-1]
    err = per_level(err_ref, levels, cols)
    odd = jnp.full((levels, cols), odd_ref[0]) == 1
    scale = jnp.where(position_ref[0] == 0, jnp.ones_like(err), err)
    for r in range(rows):
        row = r + steps
        spilled = unpack_slot(strip_ref, row, levels, steps, LANES - steps)
        value = jnp.concatenate(
            [main_ref[row, :, :-LANES], main_ref[row, :, -LANES:] + spilled], axis=1
        )
        if r < steps:
            value = value + jnp.where(odd, near_ref[r], far_ref[r])
        if r >= rows - steps:
            q = r - (rows - steps)
            value = value + jnp.where(odd, far_ref[q], near_ref[q])
        value = value + scale * (own_ref[0, r] - previous_ref[r])
        tiles = cols // LANES
        for c in range(tiles):
            out_ref[pl.ds(c * rows + r, levels, stride=rows * tiles), :] = value[:, c * LANES : (c + 1) * LANES]


def along(value, axis, by, ring=False):
    count = lax.axis_size(axis)
    if ring:
        return lax.ppermute(value, axis, [(i, (i + by) % count) for i in range(count)])
    return lax.ppermute(value, axis, [(i, i + by) for i in range(count) if 0 <= i + by < count])


def exchanged(far, near, axis):
    count = lax.axis_size(axis)
    far = lax.ppermute(far, axis, [p for i in range(1, count - 1, 2) for p in ((i, i + 1), (i + 1, i))])
    near = lax.ppermute(near, axis, [p for i in range(0, count - 1, 2) for p in ((i, i + 1), (i + 1, i))])
    return far, near


def halves(value, axis):
    count = lax.axis_size(axis)
    if count & (count - 1):
        return lax.psum(value, axis), jnp.zeros_like(value)
    distance = 1
    other = jnp.zeros_like(value)
    while distance < count:
        if distance > 1:
            value = value + other
        other = lax.ppermute(value, axis, [(i, i ^ distance) for i in range(count)])
        distance *= 2
    return value, other


def body(
    increments, advection, diffusion, departures,
    obs_weight, error_weight, penalty_weight, filter_steps, filter_weights,
):
    members = lax.axis_size("tm")
    _, steps, levels, rows, cols = departures.shape
    middle = members * steps // 2
    position = lax.axis_index("tm").astype(jnp.int32)[None]
    odd = (lax.axis_index("lat").astype(jnp.int32) % 2)[None]
    x, adv, dif, dep = (tiled(v) for v in (increments, advection, diffusion, departures))
    bind = functools.partial
    total_rows = rows + 2 * steps
    wide = cols + LANES
    halo_rows = 3 * steps - 2
    row_set = (levels, cols)

    own, far, near = call(
        bind(pack_kernel, steps, rows, levels), (odd, x, adv, dif), [SM] + [HB] * 3,
        [(3, rows) + row_set, (halo_rows,) + row_set, (halo_rows,) + row_set],
        [pltpu.VMEM((3,) + x.shape, F32), pltpu.SemaphoreType.DMA((3,))], name="pack",
    )
    far, near = exchanged(far, near, "lat")
    following = along(x, "tm", -1)

    strip_shape = (levels, LANES * lane_slots(len(wide_rows(steps, rows)), steps))
    (strip,) = call(
        bind(strip_kernel, steps, rows, levels), (odd, own, far, near), [SM] + [VM] * 3, [strip_shape], name="strip",
    )
    strip = along(strip, "lon", 1, ring=True)

    wide_shape = (total_rows, levels, wide)
    adv_w, dif_w, keep_w, forcing, filt, final = call(
        bind(forward_kernel, steps, rows, levels, middle),
        (position, odd, filter_steps, filter_weights, obs_weight, own, far, near, strip, dep),
        [SM] * 5 + [VM] * 5,
        [wide_shape] * 3 + [(steps, rows) + row_set, (rows,) + row_set, (rows,) + row_set],
        [pltpu.VMEM(wide_shape, F32)] * 2, name="forward",
    )
    filt, other = halves(filt, "tm")
    previous = along(final, "tm", 1)

    main, spill = call(
        bind(adjoint_kernel, steps, rows, levels, middle, members),
        (position, filter_steps, filter_weights, error_weight, penalty_weight, adv_w, dif_w, keep_w, forcing, filt, other, final, following),
        [SM] * 5 + [VM] * 8,
        [(total_rows,) + row_set, (levels, LANES * lane_slots(total_rows, steps))],
        [pltpu.VMEM(wide_shape, F32)] * 2 + [pltpu.VMEM((rows,) + row_set, F32)], name="adjoint",
    )
    spill = along(spill, "lon", -1, ring=True)
    far, near = call(
        bind(spill_kernel, steps, rows, levels), (odd, main, spill), [SM] + [VM] * 2, [(steps,) + row_set] * 2, name="spill",
    )
    far, near = exchanged(far, near, "lat")
    (out,) = call(
        bind(final_kernel, steps, rows, levels),
        (position, odd, error_weight, main, spill, far, near, own, previous), [SM] * 3 + [VM] * 6, [x.shape], name="final", kept=False,
    )
    return untiled(out, levels, rows, cols)[None]


def solution(mesh):
    return jax.shard_map(
        body,
        mesh=mesh,
        in_specs=(
            P("tm", None, "lat", "lon"),
            P(None, "lat", "lon"),
            P(None, "lat", "lon"),
            P("tm", None, None, "lat", "lon"),
            P(),
            P(),
            P(),
            P(),
            P(),
        ),
        out_specs=P("tm", None, "lat", "lon"),
        check_vma=False,
    )
```
